32 devices in a mesh: kern: 16 (over z, y, x), walk: 2 (over core).
Axes of the slice: x: 2, y: 2, z: 4, core: 2. Of those that a mesh axis runs over, the one named last changes fastest.
Arguments:
- walkers: float32 [8, 2048], P(None, 'walk'), may hold values from -5 to 5
- centers: float32 [8, 32768], P(None, 'kern'), may hold values from -5 to 5
- sigmas: float32 [8, 32768], P(None, 'kern'), may hold values from 0.6 to 1.5
- heights: float32 [32768], P('kern'), may hold values from 0.2 to 2
- kernel_live: int32 [16], P('kern'), may hold values from 512 to 2048, as said below
- merge_target: int32 [2048], P('walk'), may hold values from 0 to 32767, as said below
- new_sigma: float32 [8], replicated, may hold values from 0.2 to 0.6
- norm_old: float32 [1], replicated, may hold values from 0.003 to 0.03
Outputs:
- bias: float32 [2048], P('walk')
- force: float32 [8, 2048], P(None, 'walk')
- new_heights: float32 [32768], P('kern')
- new_centers: float32 [8, 32768], P(None, 'kern')
- new_sigmas: float32 [8, 32768], P(None, 'kern')
- log_norm: float32 [1], replicated
The draws below stay inside these ranges and needn't reach their ends.
Inputs may be any that keep to these rules, and one draw needn't show every extreme that they name: `kernel_live`: slots from this number up are empty; some shard is full in every draw. `merge_target`: each entry is shard * 2048 + slot with slot below that shard's kernel_live; among the 1024 walkers of one index of walk at most 128 target one shard, every shard is targeted, and some shard receives exactly 128 in every block.
All inputs are finite; a program needn't handle non-finite values.
Results may differ from the reference program's by a relative error of at most 0.0003.
Values sent between devices are 32-bit elements; how exact they have to be, the bound alone decides.
A program may use at most 64 MiB of HBM per device.

```python
import math
import jax
import jax.numpy as jnp
from jax import lax

DIMS = 8
KS = 2048
WB = 1024
KERNELS = 32768
WALKERS = 2048
N_KERN = 16
N_WALK = 2


def live_table(key):
    first, second = jax.random.split(jax.random.fold_in(key, 11))
    live_count = jax.random.randint(first, (N_KERN,), KS // 4, KS + 1)
    fullest = jax.random.randint(second, (), 0, N_KERN)
    return jnp.where(jnp.arange(N_KERN) == fullest, KS, live_count).astype(jnp.int32)


def draw_kernel_live(key, part):
    return live_table(key)


def block_shards(block_key):
    capacity = 2 * WB // N_KERN
    key_busy, key_pick, key_order = jax.random.split(block_key, 3)
    busiest = jax.random.randint(key_busy, (), 0, N_KERN)
    others = (busiest + 1 + jnp.arange(N_KERN - 1)) % N_KERN
    units = (N_KERN - 1) * (capacity - 1)
    extra = WB - capacity - (N_KERN - 1)
    picked = jax.random.permutation(key_pick, units)[:extra]
    listed = jnp.concatenate([jnp.full((capacity,), busiest), others, others[picked // (capacity - 1)]])
    return jax.random.permutation(key_order, listed)


def draw_merge_target(key, part):
    live_count = live_table(key)
    block_keys = jax.random.split(jax.random.fold_in(key, 31), N_WALK)
    shards = jax.vmap(block_shards)(block_keys).reshape(-1)
    raw_slot = jax.random.randint(jax.random.fold_in(key, 47), (WALKERS,), 0, 1 << 30)
    slot = raw_slot % live_count[shards]
    return (shards * KS + slot).astype(jnp.int32)


def levels(rng, dims, cuts, smallest, top_value):
    def one(axis_at, shards_of):
        steps = jax.random.uniform(jax.random.fold_in(jax.random.fold_in(rng, 6), axis_at), (shards_of,), jnp.float32, smallest / len(cuts), top_value / len(cuts))
        return jnp.repeat(jnp.exp(steps), dims[axis_at] // shards_of).reshape((-1,) + (1,) * (len(dims) - axis_at - 1))

    gain = one(*cuts[0])
    for cut in cuts[1:]:
        gain = gain * one(*cut)
    return gain


def noise(own_key, shape, spread, bound, cuts=(), kind=jnp.bfloat16):
    loudness = levels(own_key, shape, cuts, -0.22, 0.18) if cuts else 1.0
    values = jax.random.normal(own_key, shape, jnp.float32) * spread * loudness
    return jnp.minimum(jnp.maximum(values, -bound), bound).astype(kind)


def setup_inputs(seed: int = 0) -> dict:
    key_of = jax.random.split(jax.random.key(seed), 9)
    return {
        "walkers": noise(key_of[0], (DIMS, WALKERS), 1.0, 5.0, ((1, 2),), jnp.float32),
        "centers": noise(key_of[1], (DIMS, KERNELS), 1.0, 5.0, ((1, 16),), jnp.float32),
        "sigmas": jnp.clip(jnp.exp(math.log(1.5) - 0.9162907 * jax.random.uniform(key_of[2], (DIMS, KERNELS), jnp.float32) ** levels(key_of[2], (DIMS, KERNELS), ((1, 16),), -0.2, 0.2)), 0.6, 1.5),
        "heights": jnp.clip(jnp.exp(math.log(2.0) - 2.3025851 * jax.random.uniform(key_of[3], (KERNELS,), jnp.float32) ** levels(key_of[3], (KERNELS,), ((0, 16),), -0.2, 0.2)), 0.2, 2.0),
        "kernel_live": draw_kernel_live(jax.random.fold_in(key_of[8], 71), 0),
        "merge_target": draw_merge_target(jax.random.fold_in(key_of[8], 71), 0),
        "new_sigma": jnp.clip(jnp.exp(jax.random.uniform(key_of[6], (DIMS,), jnp.float32, math.log(0.2), math.log(0.6))), 0.2, 0.6),
        "norm_old": jnp.clip(jnp.exp(jax.random.uniform(key_of[7], (1,), jnp.float32, math.log(0.003), math.log(0.03))), 0.003, 0.03),
    }


PREFACTOR = 0.9
EPSILON = 0.01
RATE = 0.25

def reference(walkers, centers, sigmas, heights, kernel_live, merge_target, new_sigma, norm_old):
    inverse_var = 1.0 / (sigmas * sigmas)
    slot_of = jnp.arange(KERNELS, dtype=jnp.int32) % KS
    alive = (slot_of < jnp.repeat(kernel_live, KS)).astype(jnp.float32)
    kernel_feat = jnp.concatenate([-0.5 * inverse_var, centers * inverse_var, (jnp.log(heights) - 0.5 * lax.optimization_barrier(jnp.sum(centers * centers * inverse_var, 0)))[None]], 0)
    kernel_mom = jnp.concatenate([alive[None], inverse_var * alive, centers * inverse_var * alive], 0)
    walker_feat = jnp.concatenate([walkers * walkers, walkers, jnp.ones((1, WALKERS), jnp.float32)], 0)
    block_len = 1024 if KERNELS % 1024 == 0 else KS
    block_count = KERNELS // block_len

    def step(running, block_index):
        start = (block_index * block_len).astype(jnp.int32)
        feat = lax.dynamic_slice_in_dim(kernel_feat, start, block_len, 1)
        moms = lax.dynamic_slice_in_dim(kernel_mom, start, block_len, 1)
        expo = lax.dot_general(feat, walker_feat, (((0,), (0,)), ((), ())), precision=lax.Precision.HIGHEST)
        return (running + jnp.dot(moms, jnp.exp(expo), precision=lax.Precision.HIGHEST), None)
    moments, _ = lax.scan(step, jnp.zeros((17, WALKERS), jnp.float32), jnp.arange(block_count, dtype=jnp.int32))
    live_total = jnp.sum(kernel_live).astype(jnp.float32)
    density = moments[0] / live_total
    grad = (-walkers * moments[1:9] + moments[9:17]) / live_total
    norm_value = norm_old[0]
    ratio = density / norm_value + EPSILON
    bias = PREFACTOR * jnp.log(ratio)
    force = -PREFACTOR * grad / (norm_value * ratio)
    weight = jnp.exp(bias)
    log_norm = jnp.log((1.0 - RATE) * norm_old + RATE * jnp.sum(density) / WALKERS)
    target_center = centers[:, merge_target]
    offset = walkers - target_center
    feat = jnp.concatenate([weight[None], weight * offset, weight * (offset * offset + (new_sigma * new_sigma)[:, None])], 0)
    merged_sums = jax.ops.segment_sum(feat.T, merge_target, KERNELS).T
    new_heights = heights + merged_sums[0]
    delta = merged_sums[1:9] / new_heights
    new_centers = centers + delta
    new_sigmas = jnp.sqrt((heights * sigmas * sigmas + merged_sums[9:17]) / new_heights - delta * delta)
    return (bias, force, new_heights, new_centers, new_sigmas, log_norm)
```

```python
import functools
import math

import jax
import jax.numpy as jnp
from jax import lax
from jax.experimental import pallas as pl
from jax.experimental.pallas import tpu as pltpu
from jax.sharding import PartitionSpec as P

PREFACTOR = 0.9
EPSILON = 0.01
RATE = 0.25
LANES = 128
LOG2E = math.log2(math.e)
MESH = pl.DeviceIdType.MESH
F32 = jnp.float32
BF16 = jnp.bfloat16
VMEM = pl.BlockSpec(memory_space=pltpu.VMEM)
SMEM = pl.BlockSpec(memory_space=pltpu.SMEM)


def split(x):
    high = x.astype(BF16).astype(F32)
    rest = x - high
    middle = rest.astype(BF16).astype(F32)
    low = (rest - middle).astype(BF16).astype(F32)
    return high, middle, low


def sums_kernel(dims, groups, walkers_ref, centers_ref, sigmas_ref, heights_ref, live_ref,
                out_ref, own_ref, walker_feat, kernel_feat, kernel_mom, total):
    walk_len = walkers_ref.shape[1]
    shard_len = centers_ref.shape[1]
    per = dims // groups
    walkers = walkers_ref[...]
    sq_h, sq_m, sq_l = split(walkers * walkers)
    wk_h, wk_m, wk_l = split(walkers)
    h, m, l = [sq_h, wk_h], [sq_m, wk_m], [sq_l, wk_l]
    row = lax.broadcasted_iota(jnp.int32, (8, walk_len), 0)
    ones = jnp.where(row < 3, 1.0, 0.0).astype(F32)
    pad = jnp.zeros((LANES - 12 * dims - 8, walk_len), F32)
    stacked = jnp.concatenate(h + m + h + m + l + h + [ones, pad], 0)
    walker_feat[...] = stacked.T.astype(BF16)

    centers = centers_ref[...]
    sigmas = sigmas_ref[...]
    inverse_var = 1.0 / (sigmas * sigmas)
    scaled = centers * inverse_var
    constant = jnp.log(heights_ref[...]) - 0.5 * jnp.sum(centers * scaled, 0, keepdims=True)
    k_sq = split((-0.5 * LOG2E) * inverse_var)
    k_lin = split(LOG2E * scaled)
    k_con = split(LOG2E * constant)
    row = lax.broadcasted_iota(jnp.int32, (8, shard_len), 0)
    con = jnp.where(row == 0, k_con[0], jnp.where(row == 1, k_con[1], jnp.where(row == 2, k_con[2], 0.0)))
    h, m, l = [[k_sq[i], k_lin[i]] for i in range(3)]
    pad = jnp.zeros((LANES - 12 * dims - 8, shard_len), F32)
    kernel_feat[...] = jnp.concatenate(h + h + m + m + h + l + [con, pad], 0).astype(BF16)

    live = live_ref[0]
    alive = (lax.broadcasted_iota(jnp.int32, (8, shard_len), 1) < live).astype(F32)
    first = jnp.where(row == 0, alive, 0.0)
    mom_a = split(inverse_var * alive)
    mom_c = split(scaled * alive)
    pad = jnp.zeros((LANES - 6 * dims - 8, shard_len), F32)
    rows = [mom_a[0], mom_c[0], mom_a[1], mom_c[1], mom_a[2], mom_c[2], first, pad]
    kernel_mom[...] = jnp.concatenate(rows, 0).T.astype(BF16)

    block = 256
    for index in range(shard_len // block):
        part = slice(index * block, (index + 1) * block)
        expo = jnp.dot(walker_feat[...], kernel_feat[:, part], preferred_element_type=F32)
        e = jnp.exp2(expo)
        high = e.astype(BF16)
        low = (e - high.astype(F32)).astype(BF16)
        moms = kernel_mom[part, :]
        add = jnp.dot(high, moms, preferred_element_type=F32) + jnp.dot(
            low, moms, preferred_element_type=F32
        )
        if index == 0:
            total[...] = add
        else:
            total[...] += add

    moments = total[...].T
    a_sum = moments[0:dims] + moments[2 * dims : 3 * dims] + moments[4 * dims : 5 * dims]
    c_sum = moments[dims : 2 * dims] + moments[3 * dims : 4 * dims] + moments[5 * dims : 6 * dims]
    density = moments[6 * dims : 6 * dims + 1]
    live_row = jnp.full((1, LANES), live, jnp.int32).astype(F32)
    for chunk in range(walk_len // LANES):
        part = slice(chunk * LANES, (chunk + 1) * LANES)
        for group in range(groups):
            unit = chunk * groups + group
            rows = slice(group * per, (group + 1) * per)
            out_ref[unit, 0:per, :] = a_sum[rows, part]
            out_ref[unit, per : 2 * per, :] = c_sum[rows, part]
            out_ref[unit, 2 * per : 2 * per + 1, :] = density[:, part]
            out_ref[unit, 2 * per + 1 : 2 * per + 2, :] = live_row
            own_ref[unit] = walkers[rows, part]


def exchange_kernel(kern_count, walk_count, groups, sums_ref, own_ref, walkers_ref, target_ref, norm_ref,
                    share_ref, density_ref, all_walkers_ref, all_targets_ref,
                    got, mine, shared, far, far_walkers, far_targets,
                    send_a, recv_a, send_b, recv_b, send_c, recv_c, send_w, recv_w, send_t, recv_t):
    me = lax.axis_index("kern")
    walk = lax.axis_index("walk")
    per = own_ref.shape[1]
    chunks = kern_count // groups
    my_chunk = me // groups
    my_group = me % groups
    norm = norm_ref[0]

    def peer(step):
        return lax.rem(me + step, kern_count)

    def other(step):
        return lax.rem(walk + step, walk_count)

    def far_kern(index):
        return index * groups + my_group

    barrier = pltpu.get_barrier_semaphore()

    def greet(step, carry):
        pl.semaphore_signal(barrier, inc=1, device_id=(peer(step), walk), device_id_type=MESH)
        return carry

    lax.fori_loop(1, kern_count, greet, 0)
    for step in range(1, walk_count):
        def greet_far(index, carry):
            pl.semaphore_signal(
                barrier, inc=1, device_id=(far_kern(index), other(step)), device_id_type=MESH
            )
            return carry

        lax.fori_loop(0, chunks, greet_far, 0)
    pl.semaphore_wait(barrier, kern_count - 1 + (walk_count - 1) * chunks)

    def copy_a(target, source):
        return pltpu.make_async_remote_copy(
            src_ref=sums_ref.at[target], dst_ref=got.at[source],
            send_sem=send_a.at[target], recv_sem=recv_a.at[source],
            device_id=(target, walk), device_id_type=MESH,
        )

    def start_a(step, carry):
        copy_a(peer(step), me).start()
        return carry

    lax.fori_loop(1, kern_count, start_a, 0)

    def copy_w(step, source):
        return (
            pltpu.make_async_remote_copy(
                src_ref=walkers_ref, dst_ref=far_walkers.at[source],
                send_sem=send_w.at[step], recv_sem=recv_w.at[source],
                device_id=(me, other(step)), device_id_type=MESH,
            ),
            pltpu.make_async_remote_copy(
                src_ref=target_ref, dst_ref=far_targets.at[source],
                send_sem=send_t.at[step], recv_sem=recv_t.at[source],
                device_id=(me, other(step)), device_id_type=MESH,
            ),
        )

    for step in range(1, walk_count):
        for copy in copy_w(step, walk):
            copy.start()

    got[me] = sums_ref[me]
    far_walkers[walk] = walkers_ref[...]
    far_targets[walk] = target_ref[...]

    def wait_a(step, carry):
        copy_a(peer(step), peer(step)).wait_recv()
        return carry

    lax.fori_loop(1, kern_count, wait_a, 0)
    total = got[0]
    for source in range(1, kern_count):
        total = total + got[source]

    live_total = total[2 * per + 1 : 2 * per + 2]
    density = total[2 * per : 2 * per + 1] / live_total
    grad = (-own_ref[me] * total[0:per] + total[per : 2 * per]) / live_total
    ratio = density / norm + EPSILON
    force = -PREFACTOR * grad / (norm * ratio)
    mine[0:1, :] = density
    mine[1 : per + 1, :] = force
    shared[me, 0:1, :] = density
    shared[me, 1 : per + 1, :] = force

    def copy_b(target, source):
        return pltpu.make_async_remote_copy(
            src_ref=mine, dst_ref=shared.at[source],
            send_sem=send_b.at[target], recv_sem=recv_b.at[source],
            device_id=(target, walk), device_id_type=MESH,
        )

    def copy_c(step, index, chunk, source):
        return pltpu.make_async_remote_copy(
            src_ref=mine, dst_ref=far.at[source, chunk],
            send_sem=send_c.at[step, index], recv_sem=recv_c.at[source, chunk],
            device_id=(far_kern(index), other(step)), device_id_type=MESH,
        )

    for step in range(1, walk_count):
        def start_c(index, carry):
            copy_c(step, index, my_chunk, walk).start()
            return carry

        lax.fori_loop(0, chunks, start_c, 0)

    def start_b(step, carry):
        copy_b(peer(step), me).start()
        return carry

    lax.fori_loop(1, kern_count, start_b, 0)

    def wait_b(step, carry):
        copy_b(peer(step), peer(step)).wait_recv()
        return carry

    lax.fori_loop(1, kern_count, wait_b, 0)
    for chunk in range(chunks):
        far[walk, chunk] = shared[chunk * groups]
    share_ref[...] = shared[...]
    for step in range(1, walk_count):
        def wait_c(index, carry):
            copy_c(step, index, index, other(step)).wait_recv()
            return carry

        lax.fori_loop(0, chunks, wait_c, 0)
        for copy in copy_w(step, other(step)):
            copy.wait_recv()
    for block in range(walk_count):
        for chunk in range(chunks):
            density_ref[block, :, chunk * LANES : (chunk + 1) * LANES] = far[block, chunk][0:1, :]
    all_walkers_ref[...] = far_walkers[...]
    all_targets_ref[...] = far_targets[...]

    def wait_sends(step, carry):
        copy_a(peer(step), me).wait_send()
        copy_b(peer(step), me).wait_send()
        return carry

    lax.fori_loop(1, kern_count, wait_sends, 0)
    for step in range(1, walk_count):
        def wait_send_c(index, carry):
            copy_c(step, index, my_chunk, walk).wait_send()
            return carry

        lax.fori_loop(0, chunks, wait_send_c, 0)
        for copy in copy_w(step, walk):
            copy.wait_send()


def merge_kernel(groups, share_ref, density_ref, walkers_ref, targets_ref, centers_ref, sigmas_ref, heights_ref,
                 new_sigma_ref, norm_ref,
                 bias_ref, force_ref, new_heights_ref, new_centers_ref, new_sigmas_ref, log_norm_ref,
                 merged):
    dims, shard_len = centers_ref.shape
    walk_count, _, walk_len = density_ref.shape
    per = dims // groups
    chunks = walk_len // LANES
    norm = norm_ref[0]

    def biased(density):
        return PREFACTOR * jnp.log(density / norm + EPSILON)

    for chunk in range(chunks):
        part = slice(chunk * LANES, (chunk + 1) * LANES)
        bias_ref[:, part] = biased(share_ref[chunk * groups][0:1, :])
        for group in range(groups):
            force_ref[group * per : (group + 1) * per, part] = share_ref[chunk * groups + group][1 : per + 1, :]

    density_sum = jnp.zeros((1, 1), F32)
    for block in range(walk_count):
        density_sum = density_sum + jnp.sum(density_ref[block], 1, keepdims=True)
    log_norm_ref[...] = jnp.log((1.0 - RATE) * norm + RATE * density_sum / (walk_len * walk_count))

    base = lax.axis_index("kern") * shard_len
    row = lax.broadcasted_iota(jnp.int32, (8, walk_len), 0)
    tile = 256
    for block in range(walk_count):
        weight = jnp.exp(biased(density_ref[block]))
        walkers = walkers_ref[block]
        lin = split(weight * walkers)
        sq = split(weight * (walkers * walkers))
        plain = split(weight)
        last = jnp.where(row == 0, plain[0], jnp.where(row == 1, plain[1], jnp.where(row == 2, plain[2], 0.0)))
        pad = jnp.zeros((8, walk_len), F32)
        feat = jnp.concatenate(
            [lin[0], sq[0], lin[1], sq[1], lin[2], sq[2], last, pad], 0
        ).astype(BF16)
        local = targets_ref[block] - base
        for index in range(shard_len // tile):
            slot = lax.broadcasted_iota(jnp.int32, (tile, walk_len), 0) + index * tile
            placing = jnp.where(slot == local, 1.0, 0.0).astype(BF16)
            add = lax.dot_general(
                feat, placing, (((1,), (1,)), ((), ())), preferred_element_type=F32
            )
            part = slice(index * tile, (index + 1) * tile)
            if block == 0:
                merged[:, part] = add
            else:
                merged[:, part] += add

    sums = merged[...]
    first = sums[0:dims] + (sums[2 * dims : 3 * dims] + sums[4 * dims : 5 * dims])
    second = sums[dims : 2 * dims] + (sums[3 * dims : 4 * dims] + sums[5 * dims : 6 * dims])
    at = 6 * dims
    gain = sums[at : at + 1] + (sums[at + 1 : at + 2] + sums[at + 2 : at + 3])
    dim = lax.broadcasted_iota(jnp.int32, (dims, 1), 0)
    new_sigma = jnp.zeros((dims, 1), F32)
    for d in range(dims):
        new_sigma = jnp.where(dim == d, new_sigma_ref[d], new_sigma)
    centers = centers_ref[...]
    sigmas = sigmas_ref[...]
    heights = heights_ref[...]
    shift = first - centers * gain
    spread = second - 2.0 * centers * first + centers * centers * gain + new_sigma * new_sigma * gain
    new_heights = heights + gain
    delta = shift / new_heights
    new_heights_ref[...] = new_heights
    new_centers_ref[...] = centers + delta
    new_sigmas_ref[...] = jnp.sqrt((heights * sigmas * sigmas + spread) / new_heights - delta * delta)


def per_device(walkers, centers, sigmas, heights, kernel_live, merge_target, new_sigma, norm_old):
    dims, walk_len = walkers.shape
    shard_len = centers.shape[1]
    kern_count = lax.axis_size("kern")
    walk_count = lax.axis_size("walk")
    chunks = walk_len // LANES
    groups = kern_count // chunks
    per = dims // groups
    height_row = heights.reshape(1, shard_len)

    sums, own = pl.pallas_call(
        functools.partial(sums_kernel, dims, groups),
        out_shape=(
            jax.ShapeDtypeStruct((kern_count, 2 * per + 2, LANES), F32),
            jax.ShapeDtypeStruct((kern_count, per, LANES), F32),
        ),
        in_specs=[VMEM, VMEM, VMEM, VMEM, SMEM],
        out_specs=(VMEM, VMEM),
        scratch_shapes=[
            pltpu.VMEM((walk_len, LANES), BF16),
            pltpu.VMEM((LANES, shard_len), BF16),
            pltpu.VMEM((shard_len, LANES), BF16),
            pltpu.VMEM((walk_len, LANES), F32),
        ],
        name="sums",
    )(walkers, centers, sigmas, height_row, kernel_live)

    dma = pltpu.SemaphoreType.DMA
    share, density, all_walkers, all_targets = pl.pallas_call(
        functools.partial(exchange_kernel, kern_count, walk_count, groups),
        out_shape=(
            jax.ShapeDtypeStruct((kern_count, per + 1, LANES), F32),
            jax.ShapeDtypeStruct((walk_count, 1, walk_len), F32),
            jax.ShapeDtypeStruct((walk_count, dims, walk_len), F32),
            jax.ShapeDtypeStruct((walk_count, 1, walk_len), jnp.int32),
        ),
        in_specs=[VMEM, VMEM, VMEM, VMEM, SMEM],
        out_specs=(VMEM, VMEM, VMEM, VMEM),
        scratch_shapes=[
            pltpu.VMEM((kern_count, 2 * per + 2, LANES), F32),
            pltpu.VMEM((per + 1, LANES), F32),
            pltpu.VMEM((kern_count, per + 1, LANES), F32),
            pltpu.VMEM((walk_count, chunks, per + 1, LANES), F32),
            pltpu.VMEM((walk_count, dims, walk_len), F32),
            pltpu.VMEM((walk_count, 1, walk_len), jnp.int32),
            dma((kern_count,)), dma((kern_count,)),
            dma((kern_count,)), dma((kern_count,)),
            dma((walk_count, chunks)), dma((walk_count, chunks)),
            dma((walk_count,)), dma((walk_count,)),
            dma((walk_count,)), dma((walk_count,)),
        ],
        compiler_params=pltpu.CompilerParams(collective_id=0, has_side_effects=True),
        name="exchange",
    )(sums, own, walkers, merge_target.reshape(1, walk_len), norm_old)

    bias, force, new_heights, new_centers, new_sigmas, log_norm = pl.pallas_call(
        functools.partial(merge_kernel, groups),
        out_shape=(
            jax.ShapeDtypeStruct((1, walk_len), F32),
            jax.ShapeDtypeStruct((dims, walk_len), F32),
            jax.ShapeDtypeStruct((1, shard_len), F32),
            jax.ShapeDtypeStruct((dims, shard_len), F32),
            jax.ShapeDtypeStruct((dims, shard_len), F32),
            jax.ShapeDtypeStruct((1, 1), F32),
        ),
        in_specs=[VMEM] * 7 + [SMEM, SMEM],
        out_specs=(VMEM,) * 6,
        scratch_shapes=[pltpu.VMEM((6 * dims + 16, shard_len), F32)],
        name="merge",
    )(share, density, all_walkers, all_targets, centers, sigmas, height_row, new_sigma, norm_old)
    return (bias.reshape(walk_len), force, new_heights.reshape(shard_len), new_centers, new_sigmas, log_norm.reshape(1))


def solution(mesh):
    in_specs = (
        P(None, "walk"),
        P(None, "kern"),
        P(None, "kern"),
        P("kern"),
        P("kern"),
        P("walk"),
        P(),
        P(),
    )
    out_specs = (P("walk"), P(None, "walk"), P("kern"), P(None, "kern"), P(None, "kern"), P())
    return jax.shard_map(
        per_device, mesh=mesh, in_specs=in_specs, out_specs=out_specs, check_vma=False
    )
```

```python
import functools
import math

import jax
import jax.numpy as jnp
from jax import lax
from jax.experimental import pallas as pl
from jax.experimental.pallas import tpu as pltpu
from jax.sharding import PartitionSpec as P

PREFACTOR = 0.9
EPSILON = 0.01
RATE = 0.25
LANES = 128
LOG2E = math.log2(math.e)
MESH = pl.DeviceIdType.MESH
F32 = jnp.float32
BF16 = jnp.bfloat16
VMEM = pl.BlockSpec(memory_space=pltpu.VMEM)
SMEM = pl.BlockSpec(memory_space=pltpu.SMEM)


def split(x):
    high = x.astype(BF16).astype(F32)
    rest = x - high
    middle = rest.astype(BF16).astype(F32)
    low = (rest - middle).astype(BF16).astype(F32)
    return high, middle, low


def row_of(parts, width):
    row = lax.broadcasted_iota(jnp.int32, (8, width), 0)
    block = jnp.zeros((8, width), F32)
    for index, part in enumerate(parts):
        block = jnp.where(row == index, part, block)
    return block


def farthest_first(count):
    return sorted(range(count), key=lambda step: -min(step, count - step))


def sums_kernel(kern_count, walk_count, groups, capacity,
                walkers_ref, target_ref, centers_ref, sigmas_ref, heights_ref, live_ref, norm_ref,
                share_ref, density_ref, packed_ref, packed_slot_ref, packed_density_ref,
                walker_feat, kernel_feat, kernel_mom, sums, own, got, mine, shared, far,
                far_walkers, far_targets, table,
                send_a, recv_a, send_b, recv_b, send_c, recv_c, send_w, recv_w, send_t, recv_t):
    dims, walk_len = walkers_ref.shape
    shard_len = centers_ref.shape[1]
    per = dims // groups
    chunks = kern_count // groups
    me = lax.axis_index("kern")
    walk = lax.axis_index("walk")
    my_chunk = me // groups
    my_group = lax.rem(me, groups)
    norm = norm_ref[0]

    def peer(step):
        return lax.rem(me + step, kern_count)

    def other(step):
        return lax.rem(walk + step, walk_count)

    def far_kern(index):
        return index * groups + my_group

    barrier = pltpu.get_barrier_semaphore()

    def greet(step, carry):
        pl.semaphore_signal(barrier, inc=1, device_id=(peer(step), walk), device_id_type=MESH)
        return carry

    lax.fori_loop(1, kern_count, greet, 0)
    for step in range(1, walk_count):
        def greet_far(index, carry):
            pl.semaphore_signal(
                barrier, inc=1, device_id=(far_kern(index), other(step)), device_id_type=MESH
            )
            return carry

        lax.fori_loop(0, chunks, greet_far, 0)

    walkers = walkers_ref[...]
    sq_h, sq_m, sq_l = split(walkers * walkers)
    wk_h, wk_m, wk_l = split(walkers)
    h, m, l = [sq_h, wk_h], [sq_m, wk_m], [sq_l, wk_l]
    one = jnp.ones((1, walk_len), F32)
    pad = jnp.zeros((LANES - 12 * dims - 8, walk_len), F32)
    stacked = jnp.concatenate(h + m + h + m + l + h + [row_of([one] * 3, walk_len), pad], 0)
    walker_feat[...] = stacked.T.astype(BF16)

    centers = centers_ref[...]
    sigmas = sigmas_ref[...]
    inverse_var = 1.0 / (sigmas * sigmas)
    scaled = centers * inverse_var
    constant = jnp.log(heights_ref[...]) - 0.5 * jnp.sum(centers * scaled, 0, keepdims=True)
    k_sq = split((-0.5 * LOG2E) * inverse_var)
    k_lin = split(LOG2E * scaled)
    con = row_of(split(LOG2E * constant), shard_len)
    h, m, l = [[k_sq[i], k_lin[i]] for i in range(3)]
    pad = jnp.zeros((LANES - 12 * dims - 8, shard_len), F32)
    kernel_feat[...] = jnp.concatenate(h + h + m + m + h + l + [con, pad], 0).astype(BF16)

    live = live_ref[0]
    alive = (lax.broadcasted_iota(jnp.int32, (8, shard_len), 1) < live).astype(F32)
    mom_a = split(inverse_var * alive)
    mom_c = split(scaled * alive)
    pad = jnp.zeros((LANES - 6 * dims - 8, shard_len), F32)
    rows = [mom_a[0], mom_c[0], mom_a[1], mom_c[1], mom_a[2], mom_c[2], row_of([alive], shard_len), pad]
    kernel_mom[...] = jnp.concatenate(rows, 0).T.astype(BF16)

    live_row = jnp.full((1, LANES), live, jnp.int32).astype(F32)
    for unit in range(kern_count):
        chunk, group = unit // groups, unit % groups
        own[unit] = walkers[group * per : (group + 1) * per, chunk * LANES : (chunk + 1) * LANES]

    width = 2 * LANES
    quarters = walk_len // width
    units = kern_count // quarters
    block = min(512, shard_len)

    def copy_a(target, source):
        return pltpu.make_async_remote_copy(
            src_ref=sums.at[target], dst_ref=got.at[source],
            send_sem=send_a.at[target], recv_sem=recv_a.at[source],
            device_id=(target, walk), device_id_type=MESH,
        )

    def compute(step):
        quarter = lax.rem(me // units + step, quarters)
        feat = walker_feat[pl.ds(pl.multiple_of(quarter * width, width), width), :]
        total = None
        for index in range(shard_len // block):
            part = slice(index * block, (index + 1) * block)
            e = jnp.exp2(jnp.dot(feat, kernel_feat[:, part], preferred_element_type=F32))
            high = e.astype(BF16)
            low = (e - high.astype(F32)).astype(BF16)
            moms = kernel_mom[part, :]
            add = jnp.dot(high, moms, preferred_element_type=F32) + jnp.dot(
                low, moms, preferred_element_type=F32
            )
            total = add if total is None else total + add
        moments = total.T
        a_sum = moments[0:dims] + moments[2 * dims : 3 * dims] + moments[4 * dims : 5 * dims]
        c_sum = moments[dims : 2 * dims] + moments[3 * dims : 4 * dims] + moments[5 * dims : 6 * dims]
        density = moments[6 * dims : 6 * dims + 1]
        for chunk in range(2):
            part = slice(chunk * LANES, (chunk + 1) * LANES)
            for group in range(groups):
                unit = quarter * units + chunk * groups + group
                rows = slice(group * per, (group + 1) * per)
                sums[unit, 0:per, :] = a_sum[rows, part]
                sums[unit, per : 2 * per, :] = c_sum[rows, part]
                sums[unit, 2 * per : 2 * per + 1, :] = density[:, part]
                sums[unit, 2 * per + 1 : 2 * per + 2, :] = live_row

    def send(step):
        quarter = lax.rem(me // units + step, quarters)

        def start_a(index, carry):
            copy_a(quarter * units + lax.rem(me + index, units), me).start()
            return carry

        lax.fori_loop(0 if step else 1, units, start_a, 0)

    def copy_w(step, source):
        return (
            pltpu.make_async_remote_copy(
                src_ref=walkers_ref, dst_ref=far_walkers.at[source],
                send_sem=send_w.at[step], recv_sem=recv_w.at[source],
                device_id=(me, other(step)), device_id_type=MESH,
            ),
            pltpu.make_async_remote_copy(
                src_ref=target_ref, dst_ref=far_targets.at[source],
                send_sem=send_t.at[step], recv_sem=recv_t.at[source],
                device_id=(me, other(step)), device_id_type=MESH,
            ),
        )

    order = farthest_first(quarters)
    for position, step in enumerate(order):
        compute(step)
        if position == 1:
            pl.semaphore_wait(barrier, kern_count - 1 + (walk_count - 1) * chunks)
            send(order[0])
            for far_step in range(1, walk_count):
                for copy in copy_w(far_step, walk):
                    copy.start()
        if position >= 1:
            send(step)

    got[me] = sums[me]
    far_walkers[walk] = walkers
    far_targets[walk] = target_ref[...]
    for step in range(1, walk_count):
        for copy in copy_w(step, other(step)):
            copy.wait_recv()
    targets = [far_targets[index] for index in range(walk_count)]
    if walk_count % 8:
        targets.append(jnp.full((8 - walk_count % 8, walk_len), -1, jnp.int32))
    local = jnp.concatenate(targets, 0) - me * shard_len
    owned = (local >= 0) & (local < shard_len)
    before = lax.broadcasted_iota(jnp.int32, (walk_len, walk_len), 0) < lax.broadcasted_iota(
        jnp.int32, (walk_len, walk_len), 1
    )
    place = jnp.dot(
        jnp.where(owned, 1.0, 0.0).astype(BF16),
        jnp.where(before, 1.0, 0.0).astype(BF16),
        preferred_element_type=F32,
    )
    place = jnp.where(owned, place, -1.0)
    slot = jnp.where(owned, (local + 1).astype(F32), 0.0)
    want = lax.broadcasted_iota(jnp.int32, (capacity, walk_len), 0).astype(F32)

    def pack(feat, index):
        return lax.dot_general(
            feat.astype(BF16), table[index], (((1,), (1,)), ((), ())), preferred_element_type=F32
        )

    for index in range(walk_count):
        table[index] = jnp.where(want == place[index : index + 1], 1.0, 0.0).astype(BF16)
        high, middle, low = split(far_walkers[index])
        slot_rows = row_of(split(slot[index : index + 1]), walk_len)
        packed = pack(jnp.concatenate([high, middle, low, slot_rows], 0), index)
        packed_ref[index] = packed[0:dims] + (packed[dims : 2 * dims] + packed[2 * dims : 3 * dims])
        at = 3 * dims
        packed_slot_ref[index] = packed[at : at + 1] + packed[at + 1 : at + 2] + packed[at + 2 : at + 3] - 1.0

    def wait_a(step, carry):
        copy_a(peer(step), peer(step)).wait_recv()
        return carry

    lax.fori_loop(1, kern_count, wait_a, 0)
    total = got[0]
    for source in range(1, kern_count):
        total = total + got[source]

    live_total = total[2 * per + 1 : 2 * per + 2]
    density = total[2 * per : 2 * per + 1] / live_total
    grad = (-own[me] * total[0:per] + total[per : 2 * per]) / live_total
    ratio = density / norm + EPSILON
    force = -PREFACTOR * grad / (norm * ratio)
    mine[0:1, :] = density
    mine[1 : per + 1, :] = force

    def copy_b(target, source):
        return pltpu.make_async_remote_copy(
            src_ref=mine, dst_ref=shared.at[source],
            send_sem=send_b.at[target], recv_sem=recv_b.at[source],
            device_id=(target, walk), device_id_type=MESH,
        )

    def copy_c(step, index, chunk, source):
        return pltpu.make_async_remote_copy(
            src_ref=mine, dst_ref=far.at[source, chunk],
            send_sem=send_c.at[step, index], recv_sem=recv_c.at[source, chunk],
            device_id=(far_kern(index), other(step)), device_id_type=MESH,
        )

    def start_b(step, carry):
        copy_b(peer(step), me).start()
        return carry

    for step in range(1, walk_count):
        def start_c(index, carry):
            copy_c(step, lax.rem(my_chunk + index, chunks), my_chunk, walk).start()
            return carry

        half = chunks // 2
        lax.fori_loop(half, chunks, start_c, 0)
        lax.fori_loop(0, half, start_c, 0)
    lax.fori_loop(kern_count // 2, kern_count, start_b, 0)
    lax.fori_loop(1, kern_count // 2, start_b, 0)

    shared[me, 0:1, :] = density
    shared[me, 1 : per + 1, :] = force

    def wait_b(step, carry):
        copy_b(peer(step), peer(step)).wait_recv()
        return carry

    lax.fori_loop(1, kern_count, wait_b, 0)
    for chunk in range(chunks):
        far[walk, chunk] = shared[chunk * groups]
    share_ref[...] = shared[...]
    for step in range(1, walk_count):
        def wait_c(index, carry):
            copy_c(step, index, index, other(step)).wait_recv()
            return carry

        lax.fori_loop(0, chunks, wait_c, 0)
    for index in range(walk_count):
        whole = jnp.concatenate([far[index, chunk][0:1, :] for chunk in range(chunks)], 1)
        density_ref[index] = whole
        packed = pack(row_of(split(whole), walk_len), index)
        packed_density_ref[index] = packed[0:1] + packed[1:2] + packed[2:3]

    def wait_sends(step, carry):
        copy_a(peer(step), me).wait_send()
        copy_b(peer(step), me).wait_send()
        return carry

    lax.fori_loop(1, kern_count, wait_sends, 0)
    for step in range(1, walk_count):
        def wait_send_c(index, carry):
            copy_c(step, index, my_chunk, walk).wait_send()
            return carry

        lax.fori_loop(0, chunks, wait_send_c, 0)
        for copy in copy_w(step, walk):
            copy.wait_send()


def merge_kernel(groups, share_ref, density_ref, packed_ref, packed_slot_ref, packed_density_ref,
                 centers_ref, sigmas_ref, heights_ref, new_sigma_ref, norm_ref,
                 bias_ref, force_ref, new_heights_ref, new_centers_ref, new_sigmas_ref, log_norm_ref):
    dims, shard_len = centers_ref.shape
    walk_count, _, walk_len = density_ref.shape
    capacity = packed_ref.shape[2]
    per = dims // groups
    chunks = walk_len // LANES
    norm = norm_ref[0]

    def biased(density):
        return PREFACTOR * jnp.log(density / norm + EPSILON)

    for chunk in range(chunks):
        part = slice(chunk * LANES, (chunk + 1) * LANES)
        bias_ref[:, part] = biased(share_ref[chunk * groups][0:1, :])
        for group in range(groups):
            force_ref[group * per : (group + 1) * per, part] = share_ref[chunk * groups + group][1 : per + 1, :]

    density_sum = jnp.zeros((1, 1), F32)
    for index in range(walk_count):
        density_sum = density_sum + jnp.sum(density_ref[index], 1, keepdims=True)
    log_norm_ref[...] = jnp.log((1.0 - RATE) * norm + RATE * density_sum / (walk_len * walk_count))

    slots = lax.broadcasted_iota(jnp.int32, (shard_len, capacity), 0).astype(F32)
    sums = None
    for index in range(walk_count):
        weight = jnp.exp(biased(packed_density_ref[index]))
        walkers = packed_ref[index]
        lin = split(weight * walkers)
        sq = split(weight * (walkers * walkers))
        last = row_of(split(weight), capacity)
        pad = jnp.zeros((8, capacity), F32)
        feat = jnp.concatenate([lin[0], sq[0], lin[1], sq[1], lin[2], sq[2], last, pad], 0).astype(BF16)
        placing = jnp.where(slots == packed_slot_ref[index], 1.0, 0.0).astype(BF16)
        add = lax.dot_general(feat, placing, (((1,), (1,)), ((), ())), preferred_element_type=F32)
        sums = add if sums is None else sums + add

    first = sums[0:dims] + (sums[2 * dims : 3 * dims] + sums[4 * dims : 5 * dims])
    second = sums[dims : 2 * dims] + (sums[3 * dims : 4 * dims] + sums[5 * dims : 6 * dims])
    at = 6 * dims
    gain = sums[at : at + 1] + (sums[at + 1 : at + 2] + sums[at + 2 : at + 3])
    dim = lax.broadcasted_iota(jnp.int32, (dims, 1), 0)
    new_sigma = jnp.zeros((dims, 1), F32)
    for d in range(dims):
        new_sigma = jnp.where(dim == d, new_sigma_ref[d], new_sigma)
    centers = centers_ref[...]
    sigmas = sigmas_ref[...]
    heights = heights_ref[...]
    shift = first - centers * gain
    spread = second - 2.0 * centers * first + centers * centers * gain + new_sigma * new_sigma * gain
    new_heights = heights + gain
    delta = shift / new_heights
    new_heights_ref[...] = new_heights
    new_centers_ref[...] = centers + delta
    new_sigmas_ref[...] = jnp.sqrt((heights * sigmas * sigmas + spread) / new_heights - delta * delta)


def per_device(walkers, centers, sigmas, heights, kernel_live, merge_target, new_sigma, norm_old):
    dims, walk_len = walkers.shape
    shard_len = centers.shape[1]
    kern_count = lax.axis_size("kern")
    walk_count = lax.axis_size("walk")
    chunks = walk_len // LANES
    groups = kern_count // chunks
    per = dims // groups
    capacity = 2 * walk_len // kern_count
    height_row = heights.reshape(1, shard_len)

    dma = pltpu.SemaphoreType.DMA
    share, density, packed, packed_slot, packed_density = pl.pallas_call(
        functools.partial(sums_kernel, kern_count, walk_count, groups, capacity),
        out_shape=(
            jax.ShapeDtypeStruct((kern_count, per + 1, LANES), F32),
            jax.ShapeDtypeStruct((walk_count, 1, walk_len), F32),
            jax.ShapeDtypeStruct((walk_count, dims, capacity), F32),
            jax.ShapeDtypeStruct((walk_count, 1, capacity), F32),
            jax.ShapeDtypeStruct((walk_count, 1, capacity), F32),
        ),
        in_specs=[VMEM] * 5 + [SMEM, SMEM],
        out_specs=(VMEM,) * 5,
        scratch_shapes=[
            pltpu.VMEM((walk_len, LANES), BF16),
            pltpu.VMEM((LANES, shard_len), BF16),
            pltpu.VMEM((shard_len, LANES), BF16),
            pltpu.VMEM((kern_count, 2 * per + 2, LANES), F32),
            pltpu.VMEM((kern_count, per, LANES), F32),
            pltpu.VMEM((kern_count, 2 * per + 2, LANES), F32),
            pltpu.VMEM((per + 1, LANES), F32),
            pltpu.VMEM((kern_count, per + 1, LANES), F32),
            pltpu.VMEM((walk_count, chunks, per + 1, LANES), F32),
            pltpu.VMEM((walk_count, dims, walk_len), F32),
            pltpu.VMEM((walk_count, 1, walk_len), jnp.int32),
            pltpu.VMEM((walk_count, capacity, walk_len), BF16),
            dma((kern_count,)), dma((kern_count,)),
            dma((kern_count,)), dma((kern_count,)),
            dma((walk_count, chunks)), dma((walk_count, chunks)),
            dma((walk_count,)), dma((walk_count,)),
            dma((walk_count,)), dma((walk_count,)),
        ],
        compiler_params=pltpu.CompilerParams(collective_id=0, has_side_effects=True),
        name="sums",
    )(walkers, merge_target.reshape(1, walk_len), centers, sigmas, height_row, kernel_live, norm_old)

    bias, force, new_heights, new_centers, new_sigmas, log_norm = pl.pallas_call(
        functools.partial(merge_kernel, groups),
        out_shape=(
            jax.ShapeDtypeStruct((1, walk_len), F32),
            jax.ShapeDtypeStruct((dims, walk_len), F32),
            jax.ShapeDtypeStruct((1, shard_len), F32),
            jax.ShapeDtypeStruct((dims, shard_len), F32),
            jax.ShapeDtypeStruct((dims, shard_len), F32),
            jax.ShapeDtypeStruct((1, 1), F32),
        ),
        in_specs=[VMEM] * 8 + [SMEM, SMEM],
        out_specs=(VMEM,) * 6,
        name="merge",
    )(share, density, packed, packed_slot, packed_density, centers, sigmas, height_row, new_sigma, norm_old)
    return (bias.reshape(walk_len), force, new_heights.reshape(shard_len), new_centers, new_sigmas, log_norm.reshape(1))


def solution(mesh):
    in_specs = (
        P(None, "walk"),
        P(None, "kern"),
        P(None, "kern"),
        P("kern"),
        P("kern"),
        P("walk"),
        P(),
        P(),
    )
    out_specs = (P("walk"), P(None, "walk"), P("kern"), P(None, "kern"), P(None, "kern"), P())
    return jax.shard_map(
        per_device, mesh=mesh, in_specs=in_specs, out_specs=out_specs, check_vma=False
    )
```

```python
import functools
import math

import jax
import jax.numpy as jnp
from jax import lax
from jax.experimental import pallas as pl
from jax.experimental.pallas import tpu as pltpu
from jax.sharding import PartitionSpec as P

PREFACTOR = 0.9
EPSILON = 0.01
RATE = 0.25
LANES = 128
LOG2E = math.log2(math.e)
MESH = pl.DeviceIdType.MESH
F32 = jnp.float32
BF16 = jnp.bfloat16
VMEM = pl.BlockSpec(memory_space=pltpu.VMEM)
GRANT = 24 * 1024 * 1024
HBM = pl.BlockSpec(memory_space=pltpu.HBM)


def split(x):
    high = x.astype(BF16).astype(F32)
    rest = x - high
    middle = rest.astype(BF16).astype(F32)
    low = (rest - middle).astype(BF16).astype(F32)
    return high, middle, low


def row_of(parts, width):
    row = lax.broadcasted_iota(jnp.int32, (8, width), 0)
    block = jnp.zeros((8, width), F32)
    for index, part in enumerate(parts):
        block = jnp.where(row == index, part, block)
    return block


def farthest_first(count):
    return sorted(range(count), key=lambda step: -min(step, count - step))


def sums_kernel(kern_count, walk_count, groups, capacity,
                walkers_hbm, target_hbm, centers_hbm, sigmas_hbm, heights_hbm, live_hbm, norm_hbm,
                share_ref, density_ref, packed_ref, packed_slot_ref, packed_density_ref, norm_out_ref,
                walkers_ref, target_ref, centers_ref, sigmas_ref, heights_ref, live_ref, norm_ref, load_sem,
                walker_feat, kernel_feat, kernel_mom, sums, own, got, mine, shared, far,
                far_walkers, far_targets, table,
                send_a, recv_a, send_b, recv_b, send_c, recv_c, send_w, recv_w, send_t, recv_t):
    loads = [
        pltpu.make_async_copy(source, target, load_sem.at[index])
        for index, (source, target) in enumerate(
            [
                (walkers_hbm, walkers_ref),
                (centers_hbm, centers_ref),
                (sigmas_hbm, sigmas_ref),
                (heights_hbm, heights_ref),
                (live_hbm, live_ref),
                (norm_hbm, norm_ref),
                (target_hbm, target_ref),
            ]
        )
    ]
    for load in loads:
        load.start()
    dims, walk_len = walkers_ref.shape
    shard_len = centers_ref.shape[1]
    per = dims // groups
    chunks = kern_count // groups
    me = lax.axis_index("kern")
    walk = lax.axis_index("walk")
    my_chunk = me // groups
    my_group = lax.rem(me, groups)

    def peer(step):
        return lax.rem(me + step, kern_count)

    def other(step):
        return lax.rem(walk + step, walk_count)

    def far_kern(index):
        return index * groups + my_group

    barrier = pltpu.get_barrier_semaphore()

    def greet(step, carry):
        pl.semaphore_signal(barrier, inc=1, device_id=(peer(step), walk), device_id_type=MESH)
        return carry

    lax.fori_loop(1, kern_count, greet, 0)
    for step in range(1, walk_count):
        def greet_far(index, carry):
            pl.semaphore_signal(
                barrier, inc=1, device_id=(far_kern(index), other(step)), device_id_type=MESH
            )
            return carry

        lax.fori_loop(0, chunks, greet_far, 0)

    for load in loads:
        load.wait()
    norm = norm_ref[0]
    norm_out_ref[...] = jnp.full((1, 1), norm, F32)
    walkers = walkers_ref[...]
    sq_h, sq_m, sq_l = split(walkers * walkers)
    wk_h, wk_m, wk_l = split(walkers)
    h, m, l = [sq_h, wk_h], [sq_m, wk_m], [sq_l, wk_l]
    one = jnp.ones((1, walk_len), F32)
    pad = jnp.zeros((LANES - 12 * dims - 8, walk_len), F32)
    stacked = jnp.concatenate(h + m + h + m + l + h + [row_of([one] * 3, walk_len), pad], 0)
    stacked = stacked.astype(BF16)
    width = 2 * LANES
    quarters = walk_len // width
    for quarter in range(quarters):
        walker_feat[quarter] = stacked[:, quarter * width : (quarter + 1) * width]

    centers = centers_ref[...]
    sigmas = sigmas_ref[...]
    inverse_var = 1.0 / (sigmas * sigmas)
    scaled = centers * inverse_var
    constant = jnp.log(heights_ref[...]) - 0.5 * jnp.sum(centers * scaled, 0, keepdims=True)
    k_sq = split((-0.5 * LOG2E) * inverse_var)
    k_lin = split(LOG2E * scaled)
    con = row_of(split(LOG2E * constant), shard_len)
    h, m, l = [[k_sq[i], k_lin[i]] for i in range(3)]
    pad = jnp.zeros((LANES - 12 * dims - 8, shard_len), F32)
    kernel_feat[...] = jnp.concatenate(h + h + m + m + h + l + [con, pad], 0).T.astype(BF16)

    live = live_ref[0]
    alive = (lax.broadcasted_iota(jnp.int32, (8, shard_len), 1) < live).astype(F32)
    mom_a = split(inverse_var * alive)
    mom_c = split(scaled * alive)
    pad = jnp.zeros((8, shard_len), F32)
    rows = [mom_a[0], mom_c[0], mom_a[1], mom_c[1], mom_a[2], mom_c[2], row_of([alive], shard_len), pad]
    kernel_mom[...] = jnp.concatenate(rows, 0).astype(BF16)

    live_row = jnp.full((1, LANES), live, jnp.int32).astype(F32)
    for unit in range(kern_count):
        chunk, group = unit // groups, unit % groups
        own[unit] = walkers[group * per : (group + 1) * per, chunk * LANES : (chunk + 1) * LANES]

    units = kern_count // quarters
    block = min(512, shard_len)

    def copy_a(target, source):
        return pltpu.make_async_remote_copy(
            src_ref=sums.at[target], dst_ref=got.at[source],
            send_sem=send_a.at[target], recv_sem=recv_a.at[source],
            device_id=(target, walk), device_id_type=MESH,
        )

    def compute(step):
        quarter = lax.rem(me // units + step, quarters)
        feat = walker_feat[quarter]
        total = None
        for index in range(shard_len // block):
            part = slice(index * block, (index + 1) * block)
            e = jnp.exp2(jnp.dot(kernel_feat[part, :], feat, preferred_element_type=F32))
            high = e.astype(BF16)
            low = (e - high.astype(F32)).astype(BF16)
            moms = kernel_mom[:, part]
            add = jnp.dot(moms, high, preferred_element_type=F32) + jnp.dot(
                moms, low, preferred_element_type=F32
            )
            total = add if total is None else total + add
        moments = total
        a_sum = moments[0:dims] + moments[2 * dims : 3 * dims] + moments[4 * dims : 5 * dims]
        c_sum = moments[dims : 2 * dims] + moments[3 * dims : 4 * dims] + moments[5 * dims : 6 * dims]
        density = moments[6 * dims : 6 * dims + 1]
        for chunk in range(2):
            part = slice(chunk * LANES, (chunk + 1) * LANES)
            for group in range(groups):
                unit = quarter * units + chunk * groups + group
                rows = slice(group * per, (group + 1) * per)
                sums[unit, 0:per, :] = a_sum[rows, part]
                sums[unit, per : 2 * per, :] = c_sum[rows, part]
                sums[unit, 2 * per : 2 * per + 1, :] = density[:, part]
                sums[unit, 2 * per + 1 : 2 * per + 2, :] = live_row

    def send(step):
        quarter = lax.rem(me // units + step, quarters)

        def start_a(index, carry):
            copy_a(quarter * units + lax.rem(me + index, units), me).start()
            return carry

        lax.fori_loop(0 if step else 1, units, start_a, 0)

    def copy_w(step, source):
        return (
            pltpu.make_async_remote_copy(
                src_ref=walkers_ref, dst_ref=far_walkers.at[source],
                send_sem=send_w.at[step], recv_sem=recv_w.at[source],
                device_id=(me, other(step)), device_id_type=MESH,
            ),
            pltpu.make_async_remote_copy(
                src_ref=target_ref, dst_ref=far_targets.at[source],
                send_sem=send_t.at[step], recv_sem=recv_t.at[source],
                device_id=(me, other(step)), device_id_type=MESH,
            ),
        )

    order = farthest_first(quarters)
    for position, step in enumerate(order):
        compute(step)
        if position == 1:
            pl.semaphore_wait(barrier, kern_count - 1 + (walk_count - 1) * chunks)
            send(order[0])
            for far_step in range(1, walk_count):
                for copy in copy_w(far_step, walk):
                    copy.start()
        if position >= 1:
            send(step)

    got[me] = sums[me]
    def wait_a(step, carry):
        copy_a(peer(step), peer(step)).wait_recv()
        return carry

    lax.fori_loop(1, kern_count, wait_a, 0)
    total = got[0]
    for source in range(1, kern_count):
        total = total + got[source]

    live_total = total[2 * per + 1 : 2 * per + 2]
    density = total[2 * per : 2 * per + 1] / live_total
    grad = (-own[me] * total[0:per] + total[per : 2 * per]) / live_total
    ratio = density / norm + EPSILON
    force = -PREFACTOR * grad / (norm * ratio)
    mine[0:1, :] = density
    mine[1 : per + 1, :] = force

    def copy_b(target, source):
        return pltpu.make_async_remote_copy(
            src_ref=mine, dst_ref=shared.at[source],
            send_sem=send_b.at[target], recv_sem=recv_b.at[source],
            device_id=(target, walk), device_id_type=MESH,
        )

    def copy_c(step, index, chunk, source):
        return pltpu.make_async_remote_copy(
            src_ref=mine, dst_ref=far.at[source, chunk],
            send_sem=send_c.at[step, index], recv_sem=recv_c.at[source, chunk],
            device_id=(far_kern(index), other(step)), device_id_type=MESH,
        )

    def start_b(step, carry):
        copy_b(peer(step), me).start()
        return carry

    for step in range(1, walk_count):
        def start_c(index, carry):
            copy_c(step, lax.rem(my_chunk + index, chunks), my_chunk, walk).start()
            return carry

        half = chunks // 2
        lax.fori_loop(half, chunks, start_c, 0)
        lax.fori_loop(0, half, start_c, 0)
    lax.fori_loop(kern_count // 2, kern_count, start_b, 0)
    lax.fori_loop(1, kern_count // 2, start_b, 0)

    shared[me, 0:1, :] = density
    shared[me, 1 : per + 1, :] = force

    far_walkers[walk] = walkers
    far_targets[walk] = target_ref[...]
    for step in range(1, walk_count):
        for copy in copy_w(step, other(step)):
            copy.wait_recv()
    targets = [far_targets[index] for index in range(walk_count)]
    if walk_count % 8:
        targets.append(jnp.full((8 - walk_count % 8, walk_len), -1, jnp.int32))
    local = jnp.concatenate(targets, 0) - me * shard_len
    owned = (local >= 0) & (local < shard_len)
    before = lax.broadcasted_iota(jnp.int32, (walk_len, walk_len), 0) < lax.broadcasted_iota(
        jnp.int32, (walk_len, walk_len), 1
    )
    place = jnp.dot(
        jnp.where(owned, 1.0, 0.0).astype(BF16),
        jnp.where(before, 1.0, 0.0).astype(BF16),
        preferred_element_type=F32,
    )
    place = jnp.where(owned, place, -1.0)
    slot = jnp.where(owned, (local + 1).astype(F32), 0.0)
    want = lax.broadcasted_iota(jnp.int32, (capacity, walk_len), 0).astype(F32)

    def pack(feat, index):
        return lax.dot_general(
            feat.astype(BF16), table[index], (((1,), (1,)), ((), ())), preferred_element_type=F32
        )

    for index in range(walk_count):
        table[index] = jnp.where(want == place[index : index + 1], 1.0, 0.0).astype(BF16)
        high, middle, low = split(far_walkers[index])
        slot_rows = row_of(split(slot[index : index + 1]), walk_len)
        packed = pack(jnp.concatenate([high, middle, low, slot_rows], 0), index)
        packed_ref[index] = packed[0:dims] + (packed[dims : 2 * dims] + packed[2 * dims : 3 * dims])
        at = 3 * dims
        packed_slot_ref[index] = packed[at : at + 1] + packed[at + 1 : at + 2] + packed[at + 2 : at + 3] - 1.0

    def wait_b(step, carry):
        copy_b(peer(step), peer(step)).wait_recv()
        return carry

    lax.fori_loop(1, kern_count, wait_b, 0)
    for chunk in range(chunks):
        far[walk, chunk] = shared[chunk * groups]
    share_ref[...] = shared[...]
    for step in range(1, walk_count):
        def wait_c(index, carry):
            copy_c(step, index, index, other(step)).wait_recv()
            return carry

        lax.fori_loop(0, chunks, wait_c, 0)
    for index in range(walk_count):
        whole = jnp.concatenate([far[index, chunk][0:1, :] for chunk in range(chunks)], 1)
        density_ref[index] = whole
        packed = pack(row_of(split(whole), walk_len), index)
        packed_density_ref[index] = packed[0:1] + packed[1:2] + packed[2:3]

    def wait_sends(step, carry):
        copy_a(peer(step), me).wait_send()
        copy_b(peer(step), me).wait_send()
        return carry

    lax.fori_loop(1, kern_count, wait_sends, 0)
    for step in range(1, walk_count):
        def wait_send_c(index, carry):
            copy_c(step, index, my_chunk, walk).wait_send()
            return carry

        lax.fori_loop(0, chunks, wait_send_c, 0)
        for copy in copy_w(step, walk):
            copy.wait_send()


def merge_kernel(groups, share_ref, density_ref, packed_ref, packed_slot_ref, packed_density_ref,
                 centers_ref, sigmas_ref, heights_ref, new_sigma_ref, norm_ref,
                 bias_ref, force_ref, new_heights_ref, new_centers_ref, new_sigmas_ref, log_norm_ref):
    dims, shard_len = centers_ref.shape
    walk_count, _, walk_len = density_ref.shape
    capacity = packed_ref.shape[2]
    per = dims // groups
    chunks = walk_len // LANES
    norm = norm_ref[...]

    def biased(density):
        return PREFACTOR * jnp.log(density / norm + EPSILON)

    for chunk in range(chunks):
        part = slice(chunk * LANES, (chunk + 1) * LANES)
        bias_ref[:, part] = biased(share_ref[chunk * groups][0:1, :])
        for group in range(groups):
            force_ref[group * per : (group + 1) * per, part] = share_ref[chunk * groups + group][1 : per + 1, :]

    density_sum = jnp.zeros((1, 1), F32)
    for index in range(walk_count):
        density_sum = density_sum + jnp.sum(density_ref[index], 1, keepdims=True)
    log_norm_ref[...] = jnp.log((1.0 - RATE) * norm + RATE * density_sum / (walk_len * walk_count))

    slots = lax.broadcasted_iota(jnp.int32, (shard_len, capacity), 0).astype(F32)
    sums = None
    for index in range(walk_count):
        weight = jnp.exp(biased(packed_density_ref[index]))
        walkers = packed_ref[index]
        lin = split(weight * walkers)
        sq = split(weight * (walkers * walkers))
        last = row_of(split(weight), capacity)
        pad = jnp.zeros((8, capacity), F32)
        feat = jnp.concatenate([lin[0], sq[0], lin[1], sq[1], lin[2], sq[2], last, pad], 0).astype(BF16)
        placing = jnp.where(slots == packed_slot_ref[index], 1.0, 0.0).astype(BF16)
        add = lax.dot_general(feat, placing, (((1,), (1,)), ((), ())), preferred_element_type=F32)
        sums = add if sums is None else sums + add

    first = sums[0:dims] + (sums[2 * dims : 3 * dims] + sums[4 * dims : 5 * dims])
    second = sums[dims : 2 * dims] + (sums[3 * dims : 4 * dims] + sums[5 * dims : 6 * dims])
    at = 6 * dims
    gain = sums[at : at + 1] + (sums[at + 1 : at + 2] + sums[at + 2 : at + 3])
    row = lax.broadcasted_iota(jnp.int32, (dims, dims), 0)
    column = lax.broadcasted_iota(jnp.int32, (dims, dims), 1)
    new_sigma = jnp.sum(jnp.where(row == column, new_sigma_ref[...], 0.0), 1, keepdims=True)
    centers = centers_ref[...]
    sigmas = sigmas_ref[...]
    heights = heights_ref[...]
    shift = first - centers * gain
    spread = second - 2.0 * centers * first + centers * centers * gain + new_sigma * new_sigma * gain
    new_heights = heights + gain
    delta = shift / new_heights
    new_heights_ref[...] = new_heights
    new_centers_ref[...] = centers + delta
    new_sigmas_ref[...] = jnp.sqrt((heights * sigmas * sigmas + spread) / new_heights - delta * delta)


def per_device(walkers, centers, sigmas, heights, kernel_live, merge_target, new_sigma, norm_old):
    dims, walk_len = walkers.shape
    shard_len = centers.shape[1]
    kern_count = lax.axis_size("kern")
    walk_count = lax.axis_size("walk")
    chunks = walk_len // LANES
    groups = kern_count // chunks
    per = dims // groups
    capacity = 2 * walk_len // kern_count
    height_row = heights.reshape(1, shard_len)

    dma = pltpu.SemaphoreType.DMA
    share, density, packed, packed_slot, packed_density, norm_row = pl.pallas_call(
        functools.partial(sums_kernel, kern_count, walk_count, groups, capacity),
        out_shape=(
            jax.ShapeDtypeStruct((kern_count, per + 1, LANES), F32),
            jax.ShapeDtypeStruct((walk_count, 1, walk_len), F32),
            jax.ShapeDtypeStruct((walk_count, dims, capacity), F32),
            jax.ShapeDtypeStruct((walk_count, 1, capacity), F32),
            jax.ShapeDtypeStruct((walk_count, 1, capacity), F32),
            jax.ShapeDtypeStruct((1, 1), F32),
        ),
        in_specs=[HBM] * 7,
        out_specs=(VMEM,) * 6,
        scratch_shapes=[
            pltpu.VMEM((dims, walk_len), F32),
            pltpu.VMEM((1, walk_len), jnp.int32),
            pltpu.VMEM((dims, shard_len), F32),
            pltpu.VMEM((dims, shard_len), F32),
            pltpu.VMEM((1, shard_len), F32),
            pltpu.SMEM((1,), jnp.int32),
            pltpu.SMEM((1,), F32),
            dma((7,)),
            pltpu.VMEM((walk_len // (2 * LANES), LANES, 2 * LANES), BF16),
            pltpu.VMEM((shard_len, LANES), BF16),
            pltpu.VMEM((6 * dims + 16, shard_len), BF16),
            pltpu.VMEM((kern_count, 2 * per + 2, LANES), F32),
            pltpu.VMEM((kern_count, per, LANES), F32),
            pltpu.VMEM((kern_count, 2 * per + 2, LANES), F32),
            pltpu.VMEM((per + 1, LANES), F32),
            pltpu.VMEM((kern_count, per + 1, LANES), F32),
            pltpu.VMEM((walk_count, chunks, per + 1, LANES), F32),
            pltpu.VMEM((walk_count, dims, walk_len), F32),
            pltpu.VMEM((walk_count, 1, walk_len), jnp.int32),
            pltpu.VMEM((walk_count, capacity, walk_len), BF16),
            dma((kern_count,)), dma((kern_count,)),
            dma((kern_count,)), dma((kern_count,)),
            dma((walk_count, chunks)), dma((walk_count, chunks)),
            dma((walk_count,)), dma((walk_count,)),
            dma((walk_count,)), dma((walk_count,)),
        ],
        compiler_params=pltpu.CompilerParams(collective_id=0, has_side_effects=True),
        name="sums",
    )(walkers, merge_target.reshape(1, walk_len), centers, sigmas, height_row, kernel_live, norm_old)

    bias, force, new_heights, new_centers, new_sigmas, log_norm = pl.pallas_call(
        functools.partial(merge_kernel, groups),
        out_shape=(
            jax.ShapeDtypeStruct((1, walk_len), F32),
            jax.ShapeDtypeStruct((dims, walk_len), F32),
            jax.ShapeDtypeStruct((1, shard_len), F32),
            jax.ShapeDtypeStruct((dims, shard_len), F32),
            jax.ShapeDtypeStruct((dims, shard_len), F32),
            jax.ShapeDtypeStruct((1, 1), F32),
        ),
        in_specs=[VMEM] * 10,
        out_specs=(VMEM,) * 6,
        compiler_params=pltpu.CompilerParams(vmem_limit_bytes=GRANT),
        name="merge",
    )(share, density, packed, packed_slot, packed_density, centers, sigmas, height_row, new_sigma.reshape(1, dims), norm_row)
    return (bias.reshape(walk_len), force, new_heights.reshape(shard_len), new_centers, new_sigmas, log_norm.reshape(1))


def solution(mesh):
    in_specs = (
        P(None, "walk"),
        P(None, "kern"),
        P(None, "kern"),
        P("kern"),
        P("kern"),
        P("walk"),
        P(),
        P(),
    )
    out_specs = (P("walk"), P(None, "walk"), P("kern"), P(None, "kern"), P(None, "kern"), P())
    return jax.shard_map(
        per_device, mesh=mesh, in_specs=in_specs, out_specs=out_specs, check_vma=False
    )
```

```python
import functools
import math

import jax
import jax.numpy as jnp
from jax import lax
from jax.experimental import pallas as pl
from jax.experimental.pallas import tpu as pltpu
from jax.sharding import PartitionSpec as P

PREFACTOR = 0.9
EPSILON = 0.01
RATE = 0.25
LANES = 128
LOG2E = math.log2(math.e)
MESH = pl.DeviceIdType.MESH
F32 = jnp.float32
BF16 = jnp.bfloat16
VMEM = pl.BlockSpec(memory_space=pltpu.VMEM)
HBM = pl.BlockSpec(memory_space=pltpu.HBM)


def split(x):
    high = x.astype(BF16).astype(F32)
    rest = x - high
    middle = rest.astype(BF16).astype(F32)
    low = (rest - middle).astype(BF16).astype(F32)
    return high, middle, low


def row_of(parts, width):
    row = lax.broadcasted_iota(jnp.int32, (8, width), 0)
    block = jnp.zeros((8, width), F32)
    for index, part in enumerate(parts):
        block = jnp.where(row == index, part, block)
    return block


def farthest_first(count):
    return sorted(range(count), key=lambda step: -min(step, count - step))


def sums_kernel(kern_count, walk_count, groups, capacity,
                walkers_hbm, target_hbm, centers_hbm, sigmas_hbm, heights_hbm, live_hbm, norm_hbm,
                share_ref, density_ref, packed_ref, packed_slot_ref, packed_density_ref, norm_out_ref,
                walkers_ref, target_ref, centers_ref, sigmas_ref, heights_ref, live_ref, norm_ref, load_sem,
                walker_feat, kernel_feat, kernel_mom, sums, own, got, mine, shared, far,
                far_walkers, far_targets, table,
                send_a, recv_a, send_b, recv_b, send_c, recv_c, send_w, recv_w, send_t, recv_t):
    loads = [
        pltpu.make_async_copy(source, target, load_sem.at[index])
        for index, (source, target) in enumerate(
            [
                (walkers_hbm, walkers_ref),
                (centers_hbm, centers_ref),
                (sigmas_hbm, sigmas_ref),
                (heights_hbm, heights_ref),
                (live_hbm, live_ref),
                (norm_hbm, norm_ref),
                (target_hbm, target_ref),
            ]
        )
    ]
    for load in loads:
        load.start()
    dims, walk_len = walkers_ref.shape
    shard_len = centers_ref.shape[1]
    per = dims // groups
    chunks = kern_count // groups
    me = lax.axis_index("kern")
    walk = lax.axis_index("walk")
    my_chunk = me // groups
    my_group = lax.rem(me, groups)

    def peer(step):
        return lax.rem(me + step, kern_count)

    def other(step):
        return lax.rem(walk + step, walk_count)

    def far_kern(index):
        return index * groups + my_group

    barrier = pltpu.get_barrier_semaphore()

    def greet(step, carry):
        pl.semaphore_signal(barrier, inc=1, device_id=(peer(step), walk), device_id_type=MESH)
        return carry

    lax.fori_loop(1, kern_count, greet, 0)
    for step in range(1, walk_count):
        def greet_far(index, carry):
            pl.semaphore_signal(
                barrier, inc=1, device_id=(far_kern(index), other(step)), device_id_type=MESH
            )
            return carry

        lax.fori_loop(0, chunks, greet_far, 0)

    for load in loads:
        load.wait()
    norm = norm_ref[0]
    norm_out_ref[...] = jnp.full((1, 1), norm, F32)
    walkers = walkers_ref[...]
    sq_h, sq_m, sq_l = split(walkers * walkers)
    wk_h, wk_m, wk_l = split(walkers)
    h, m, l = [sq_h, wk_h], [sq_m, wk_m], [sq_l, wk_l]
    one = jnp.ones((1, walk_len), F32)
    pad = jnp.zeros((LANES - 12 * dims - 8, walk_len), F32)
    stacked = jnp.concatenate(h + m + h + m + l + h + [row_of([one] * 3, walk_len), pad], 0)
    stacked = stacked.astype(BF16)
    width = 2 * LANES
    quarters = walk_len // width
    for quarter in range(quarters):
        walker_feat[quarter] = stacked[:, quarter * width : (quarter + 1) * width]

    centers = centers_ref[...]
    sigmas = sigmas_ref[...]
    inverse_var = 1.0 / (sigmas * sigmas)
    scaled = centers * inverse_var
    constant = jnp.log(heights_ref[...]) - 0.5 * jnp.sum(centers * scaled, 0, keepdims=True)
    k_sq = split((-0.5 * LOG2E) * inverse_var)
    k_lin = split(LOG2E * scaled)
    con = row_of(split(LOG2E * constant), shard_len)
    h, m, l = [[k_sq[i], k_lin[i]] for i in range(3)]
    pad = jnp.zeros((LANES - 12 * dims - 8, shard_len), F32)
    kernel_feat[...] = jnp.concatenate(h + h + m + m + h + l + [con, pad], 0).T.astype(BF16)

    live = live_ref[0]
    alive = (lax.broadcasted_iota(jnp.int32, (8, shard_len), 1) < live).astype(F32)
    mom_a = split(inverse_var * alive)
    mom_c = split(scaled * alive)
    pad = jnp.zeros((8, shard_len), F32)
    rows = [mom_a[0], mom_c[0], mom_a[1], mom_c[1], mom_a[2], mom_c[2], row_of([alive], shard_len), pad]
    kernel_mom[...] = jnp.concatenate(rows, 0).astype(BF16)

    live_row = jnp.full((1, LANES), live, jnp.int32).astype(F32)
    for unit in range(kern_count):
        chunk, group = unit // groups, unit % groups
        own[unit] = walkers[group * per : (group + 1) * per, chunk * LANES : (chunk + 1) * LANES]

    units = kern_count // quarters
    block = min(512, shard_len)

    def copy_a(target, source):
        return pltpu.make_async_remote_copy(
            src_ref=sums.at[target], dst_ref=got.at[source],
            send_sem=send_a.at[target], recv_sem=recv_a.at[source],
            device_id=(target, walk), device_id_type=MESH,
        )

    def compute(step):
        quarter = lax.rem(me // units + step, quarters)
        feat = walker_feat[quarter]
        total = None
        for index in range(shard_len // block):
            part = slice(index * block, (index + 1) * block)
            e = jnp.exp2(jnp.dot(kernel_feat[part, :], feat, preferred_element_type=F32))
            high = e.astype(BF16)
            low = (e - high.astype(F32)).astype(BF16)
            moms = kernel_mom[:, part]
            add = jnp.dot(moms, high, preferred_element_type=F32) + jnp.dot(
                moms, low, preferred_element_type=F32
            )
            total = add if total is None else total + add
        moments = total
        a_sum = moments[0:dims] + moments[2 * dims : 3 * dims] + moments[4 * dims : 5 * dims]
        c_sum = moments[dims : 2 * dims] + moments[3 * dims : 4 * dims] + moments[5 * dims : 6 * dims]
        density = moments[6 * dims : 6 * dims + 1]
        for chunk in range(2):
            part = slice(chunk * LANES, (chunk + 1) * LANES)
            for group in range(groups):
                unit = quarter * units + chunk * groups + group
                rows = slice(group * per, (group + 1) * per)
                sums[unit, 0:per, :] = a_sum[rows, part]
                sums[unit, per : 2 * per, :] = c_sum[rows, part]
                sums[unit, 2 * per : 2 * per + 1, :] = density[:, part]
                sums[unit, 2 * per + 1 : 2 * per + 2, :] = live_row

    def send(step):
        quarter = lax.rem(me // units + step, quarters)

        def start_a(index, carry):
            copy_a(quarter * units + lax.rem(me + index, units), me).start()
            return carry

        lax.fori_loop(0 if step else 1, units, start_a, 0)

    def copy_w(step, source):
        return (
            pltpu.make_async_remote_copy(
                src_ref=walkers_ref, dst_ref=far_walkers.at[source],
                send_sem=send_w.at[step], recv_sem=recv_w.at[source],
                device_id=(me, other(step)), device_id_type=MESH,
            ),
            pltpu.make_async_remote_copy(
                src_ref=target_ref, dst_ref=far_targets.at[source],
                send_sem=send_t.at[step], recv_sem=recv_t.at[source],
                device_id=(me, other(step)), device_id_type=MESH,
            ),
        )

    order = farthest_first(quarters)
    for position, step in enumerate(order):
        compute(step)
        if position == 1:
            pl.semaphore_wait(barrier, kern_count - 1 + (walk_count - 1) * chunks)
            send(order[0])
            for far_step in range(1, walk_count):
                for copy in copy_w(far_step, walk):
                    copy.start()
        if position >= 1:
            send(step)

    got[me] = sums[me]
    def wait_a(step, carry):
        copy_a(peer(step), peer(step)).wait_recv()
        return carry

    lax.fori_loop(1, kern_count, wait_a, 0)
    total = got[0]
    for source in range(1, kern_count):
        total = total + got[source]

    live_total = total[2 * per + 1 : 2 * per + 2]
    density = total[2 * per : 2 * per + 1] / live_total
    grad = (-own[me] * total[0:per] + total[per : 2 * per]) / live_total
    ratio = density / norm + EPSILON
    force = -PREFACTOR * grad / (norm * ratio)
    mine[0:1, :] = density
    mine[1 : per + 1, :] = force

    def copy_b(target, source):
        return pltpu.make_async_remote_copy(
            src_ref=mine, dst_ref=shared.at[source],
            send_sem=send_b.at[target], recv_sem=recv_b.at[source],
            device_id=(target, walk), device_id_type=MESH,
        )

    def copy_c(step, index, chunk, source):
        return pltpu.make_async_remote_copy(
            src_ref=mine, dst_ref=far.at[source, chunk],
            send_sem=send_c.at[step, index], recv_sem=recv_c.at[source, chunk],
            device_id=(far_kern(index), other(step)), device_id_type=MESH,
        )

    def start_b(step, carry):
        copy_b(peer(step), me).start()
        return carry

    for step in range(1, walk_count):
        def start_c(index, carry):
            copy_c(step, lax.rem(my_chunk + index, chunks), my_chunk, walk).start()
            return carry

        half = chunks // 2
        lax.fori_loop(half, chunks, start_c, 0)
        lax.fori_loop(0, half, start_c, 0)
    lax.fori_loop(kern_count // 2, kern_count, start_b, 0)
    lax.fori_loop(1, kern_count // 2, start_b, 0)

    shared[me, 0:1, :] = density
    shared[me, 1 : per + 1, :] = force

    far_walkers[walk] = walkers
    far_targets[walk] = target_ref[...]
    for step in range(1, walk_count):
        for copy in copy_w(step, other(step)):
            copy.wait_recv()
    targets = [far_targets[index] for index in range(walk_count)]
    if walk_count % 8:
        targets.append(jnp.full((8 - walk_count % 8, walk_len), -1, jnp.int32))
    local = jnp.concatenate(targets, 0) - me * shard_len
    owned = (local >= 0) & (local < shard_len)
    before = lax.broadcasted_iota(jnp.int32, (walk_len, walk_len), 0) < lax.broadcasted_iota(
        jnp.int32, (walk_len, walk_len), 1
    )
    place = jnp.dot(
        jnp.where(owned, 1.0, 0.0).astype(BF16),
        jnp.where(before, 1.0, 0.0).astype(BF16),
        preferred_element_type=F32,
    )
    place = jnp.where(owned, place, -1.0)
    slot = jnp.where(owned, (local + 1).astype(F32), 0.0)
    want = lax.broadcasted_iota(jnp.int32, (capacity, walk_len), 0).astype(F32)

    def pack(feat, index):
        return lax.dot_general(
            feat.astype(BF16), table[index], (((1,), (1,)), ((), ())), preferred_element_type=F32
        )

    for index in range(walk_count):
        table[index] = jnp.where(want == place[index : index + 1], 1.0, 0.0).astype(BF16)
        high, middle, low = split(far_walkers[index])
        slot_rows = row_of(split(slot[index : index + 1]), walk_len)
        packed = pack(jnp.concatenate([high, middle, low, slot_rows], 0), index)
        packed_ref[index] = packed[0:dims] + (packed[dims : 2 * dims] + packed[2 * dims : 3 * dims])
        at = 3 * dims
        packed_slot_ref[index] = packed[at : at + 1] + packed[at + 1 : at + 2] + packed[at + 2 : at + 3] - 1.0

    def wait_b(step, carry):
        copy_b(peer(step), peer(step)).wait_recv()
        return carry

    lax.fori_loop(1, kern_count, wait_b, 0)
    for chunk in range(chunks):
        far[walk, chunk] = shared[chunk * groups]
    share_ref[...] = shared[...]
    for step in range(1, walk_count):
        def wait_c(index, carry):
            copy_c(step, index, index, other(step)).wait_recv()
            return carry

        lax.fori_loop(0, chunks, wait_c, 0)
    for index in range(walk_count):
        whole = jnp.concatenate([far[index, chunk][0:1, :] for chunk in range(chunks)], 1)
        density_ref[index] = whole
        packed = pack(row_of(split(whole), walk_len), index)
        packed_density_ref[index] = packed[0:1] + packed[1:2] + packed[2:3]

    def wait_sends(step, carry):
        copy_a(peer(step), me).wait_send()
        copy_b(peer(step), me).wait_send()
        return carry

    lax.fori_loop(1, kern_count, wait_sends, 0)
    for step in range(1, walk_count):
        def wait_send_c(index, carry):
            copy_c(step, index, my_chunk, walk).wait_send()
            return carry

        lax.fori_loop(0, chunks, wait_send_c, 0)
        for copy in copy_w(step, walk):
            copy.wait_send()


def merge_kernel(groups, share_ref, density_ref, packed_ref, packed_slot_ref, packed_density_ref,
                 centers_ref, sigmas_ref, heights_ref, new_sigma_ref, norm_ref,
                 bias_ref, force_ref, new_heights_ref, new_centers_ref, new_sigmas_ref, log_norm_ref):
    dims, shard_len = centers_ref.shape
    walk_count, _, walk_len = density_ref.shape
    capacity = packed_ref.shape[2]
    per = dims // groups
    chunks = walk_len // LANES
    norm = norm_ref[...]

    def biased(density):
        return PREFACTOR * jnp.log(density / norm + EPSILON)

    for chunk in range(chunks):
        part = slice(chunk * LANES, (chunk + 1) * LANES)
        bias_ref[:, part] = biased(share_ref[chunk * groups][0:1, :])
        for group in range(groups):
            force_ref[group * per : (group + 1) * per, part] = share_ref[chunk * groups + group][1 : per + 1, :]

    density_sum = jnp.zeros((1, 1), F32)
    for index in range(walk_count):
        density_sum = density_sum + jnp.sum(density_ref[index], 1, keepdims=True)
    log_norm_ref[...] = jnp.log((1.0 - RATE) * norm + RATE * density_sum / (walk_len * walk_count))

    slots = lax.broadcasted_iota(jnp.int32, (shard_len, capacity), 0).astype(F32)
    sums = None
    for index in range(walk_count):
        weight = jnp.exp(biased(packed_density_ref[index]))
        walkers = packed_ref[index]
        lin = split(weight * walkers)
        sq = split(weight * (walkers * walkers))
        last = row_of(split(weight), capacity)
        pad = jnp.zeros((8, capacity), F32)
        feat = jnp.concatenate([lin[0], sq[0], lin[1], sq[1], lin[2], sq[2], last, pad], 0).astype(BF16)
        placing = jnp.where(slots == packed_slot_ref[index], 1.0, 0.0).astype(BF16)
        add = lax.dot_general(feat, placing, (((1,), (1,)), ((), ())), preferred_element_type=F32)
        sums = add if sums is None else sums + add

    first = sums[0:dims] + (sums[2 * dims : 3 * dims] + sums[4 * dims : 5 * dims])
    second = sums[dims : 2 * dims] + (sums[3 * dims : 4 * dims] + sums[5 * dims : 6 * dims])
    at = 6 * dims
    gain = sums[at : at + 1] + (sums[at + 1 : at + 2] + sums[at + 2 : at + 3])
    row = lax.broadcasted_iota(jnp.int32, (dims, dims), 0)
    column = lax.broadcasted_iota(jnp.int32, (dims, dims), 1)
    new_sigma = jnp.sum(jnp.where(row == column, new_sigma_ref[...], 0.0), 1, keepdims=True)
    centers = centers_ref[...]
    sigmas = sigmas_ref[...]
    heights = heights_ref[...]
    shift = first - centers * gain
    spread = second - 2.0 * centers * first + centers * centers * gain + new_sigma * new_sigma * gain
    new_heights = heights + gain
    delta = shift / new_heights
    new_heights_ref[...] = new_heights
    new_centers_ref[...] = centers + delta
    new_sigmas_ref[...] = jnp.sqrt((heights * sigmas * sigmas + spread) / new_heights - delta * delta)


def per_device(walkers, centers, sigmas, heights, kernel_live, merge_target, new_sigma, norm_old):
    dims, walk_len = walkers.shape
    shard_len = centers.shape[1]
    kern_count = lax.axis_size("kern")
    walk_count = lax.axis_size("walk")
    chunks = walk_len // LANES
    groups = kern_count // chunks
    per = dims // groups
    capacity = 2 * walk_len // kern_count
    height_row = heights.reshape(1, shard_len)

    dma = pltpu.SemaphoreType.DMA
    share, density, packed, packed_slot, packed_density, norm_row = pl.pallas_call(
        functools.partial(sums_kernel, kern_count, walk_count, groups, capacity),
        out_shape=(
            jax.ShapeDtypeStruct((kern_count, per + 1, LANES), F32),
            jax.ShapeDtypeStruct((walk_count, 1, walk_len), F32),
            jax.ShapeDtypeStruct((walk_count, dims, capacity), F32),
            jax.ShapeDtypeStruct((walk_count, 1, capacity), F32),
            jax.ShapeDtypeStruct((walk_count, 1, capacity), F32),
            jax.ShapeDtypeStruct((1, 1), F32),
        ),
        in_specs=[HBM] * 7,
        out_specs=(VMEM,) * 6,
        scratch_shapes=[
            pltpu.VMEM((dims, walk_len), F32),
            pltpu.VMEM((1, walk_len), jnp.int32),
            pltpu.VMEM((dims, shard_len), F32),
            pltpu.VMEM((dims, shard_len), F32),
            pltpu.VMEM((1, shard_len), F32),
            pltpu.SMEM((1,), jnp.int32),
            pltpu.SMEM((1,), F32),
            dma((7,)),
            pltpu.VMEM((walk_len // (2 * LANES), LANES, 2 * LANES), BF16),
            pltpu.VMEM((shard_len, LANES), BF16),
            pltpu.VMEM((6 * dims + 16, shard_len), BF16),
            pltpu.VMEM((kern_count, 2 * per + 2, LANES), F32),
            pltpu.VMEM((kern_count, per, LANES), F32),
            pltpu.VMEM((kern_count, 2 * per + 2, LANES), F32),
            pltpu.VMEM((per + 1, LANES), F32),
            pltpu.VMEM((kern_count, per + 1, LANES), F32),
            pltpu.VMEM((walk_count, chunks, per + 1, LANES), F32),
            pltpu.VMEM((walk_count, dims, walk_len), F32),
            pltpu.VMEM((walk_count, 1, walk_len), jnp.int32),
            pltpu.VMEM((walk_count, capacity, walk_len), BF16),
            dma((kern_count,)), dma((kern_count,)),
            dma((kern_count,)), dma((kern_count,)),
            dma((walk_count, chunks)), dma((walk_count, chunks)),
            dma((walk_count,)), dma((walk_count,)),
            dma((walk_count,)), dma((walk_count,)),
        ],
        compiler_params=pltpu.CompilerParams(collective_id=0, has_side_effects=True),
        name="sums",
    )(walkers, merge_target.reshape(1, walk_len), centers, sigmas, height_row, kernel_live, norm_old)

    bias, force, new_heights, new_centers, new_sigmas, log_norm = pl.pallas_call(
        functools.partial(merge_kernel, groups),
        out_shape=(
            jax.ShapeDtypeStruct((1, walk_len), F32),
            jax.ShapeDtypeStruct((dims, walk_len), F32),
            jax.ShapeDtypeStruct((1, shard_len), F32),
            jax.ShapeDtypeStruct((dims, shard_len), F32),
            jax.ShapeDtypeStruct((dims, shard_len), F32),
            jax.ShapeDtypeStruct((1, 1), F32),
        ),
        in_specs=[VMEM] * 10,
        out_specs=(VMEM,) * 6,
        name="merge",
    )(share, density, packed, packed_slot, packed_density, centers, sigmas, height_row, new_sigma.reshape(1, dims), norm_row)
    return (bias.reshape(walk_len), force, new_heights.reshape(shard_len), new_centers, new_sigmas, log_norm.reshape(1))


def solution(mesh):
    in_specs = (
        P(None, "walk"),
        P(None, "kern"),
        P(None, "kern"),
        P("kern"),
        P("kern"),
        P("walk"),
        P(),
        P(),
    )
    out_specs = (P("walk"), P(None, "walk"), P("kern"), P(None, "kern"), P(None, "kern"), P())
    return jax.shard_map(
        per_device, mesh=mesh, in_specs=in_specs, out_specs=out_specs, check_vma=False
    )
```
